16 devices in a mesh: dp: 2 (over y, z), tp: 8 (over x, core).
Axes of the slice: x: 4, y: 2, z: 1, core: 2. Of those that a mesh axis runs over, the one named last changes fastest.
The devices are a block of a 4x4x8 slice.
Arguments:
- hidden: bfloat16 [12, 6, 3072], P('dp'), parts along dimension 0
- draft_ids: int32 [12, 5], P('dp'), parts along dimension 0
- temperature: float32 [12], P('dp'), parts along dimension 0
- norm_gain: bfloat16 [3072], replicated
- head_weight: bfloat16 [128256, 3072], P('tp')
Outputs:
- output 1: float32 [12, 5], P('dp'), parts along dimension 0
- output 2: float32 [12, 6], P('dp'), parts along dimension 0
- output 3: float32 [12, 6], P('dp'), parts along dimension 0
There are 2 independent parts. The reference program is written for one: setup_inputs(seed, part) draws one part's arguments, and reference() takes and returns one part's arrays. A program takes and returns all parts, laid end to end along the dimension named above; an argument that names none is the same for every part.
All inputs are finite; a program needn't handle non-finite values.
Results may differ from the reference program's by a relative error of at most 0.001.
Values sent between devices are 32-bit elements.
A program may use at most 768 MiB of HBM per device.

```python
import jax
import jax.numpy as jnp
from jax import lax

BATCH_ROWS = 6
DRAFT_LEN = 5
MODEL_DIM = 3072
VOCAB_SIZE = 128256
NORM_EPS = 1e-5


def setup_inputs(seed: int = 0, part: int = 0) -> dict:
    base_key = jax.random.key(seed)
    part_key = jax.random.fold_in(base_key, part)
    key_hidden, key_draft, key_temp = jax.random.split(part_key, 3)
    key_gain, key_head = jax.random.split(jax.random.key(seed + 1), 2)
    hidden = jax.random.normal(key_hidden, (BATCH_ROWS, DRAFT_LEN + 1, MODEL_DIM), jnp.float32).astype(jnp.bfloat16)
    draft_ids = jax.random.randint(key_draft, (BATCH_ROWS, DRAFT_LEN), 0, VOCAB_SIZE, jnp.int32)
    draft_ids = draft_ids.at[0, 0].set(0).at[0, 1].set(VOCAB_SIZE - 1)
    temperature = jax.random.uniform(key_temp, (BATCH_ROWS,), jnp.float32, 0.6, 1.2)
    norm_gain = (1.5 + 0.3 * jax.random.normal(key_gain, (MODEL_DIM,), jnp.float32)).astype(jnp.bfloat16)
    head_weight = (2.0 * MODEL_DIM ** -0.5 * jax.random.normal(key_head, (VOCAB_SIZE, MODEL_DIM), jnp.float32)).astype(jnp.bfloat16)
    return {"hidden": hidden, "draft_ids": draft_ids, "temperature": temperature, "norm_gain": norm_gain, "head_weight": head_weight}


def reference(hidden, draft_ids, temperature, norm_gain, head_weight):
    hidden_f32 = hidden.astype(jnp.float32)
    mean_sq = jnp.mean(hidden_f32 * hidden_f32, axis=-1, keepdims=True)
    normed = (hidden_f32 * lax.rsqrt(mean_sq + NORM_EPS) * norm_gain.astype(jnp.float32)).astype(jnp.bfloat16)

    def per_row(row_args):
        normed_row, draft_row, temp_row = row_args
        logits = jnp.dot(normed_row, head_weight.T, preferred_element_type=jnp.float32) / temp_row
        row_max = jnp.max(logits, axis=-1, keepdims=True)
        shifted = jnp.exp(logits - row_max)
        total = jnp.sum(shifted, axis=-1)
        weighted = jnp.sum(shifted * logits, axis=-1)
        log_norm = row_max[:, 0] + jnp.log(total)
        entropy = log_norm - weighted / total
        picked = jnp.take_along_axis(logits[:DRAFT_LEN], draft_row[:, None], axis=1)[:, 0]
        return picked - log_norm[:DRAFT_LEN], log_norm, entropy

    log_probs, log_norm, entropy = lax.map(per_row, (normed, draft_ids, temperature))
    return log_probs, log_norm, entropy
```

```python
import functools

import jax
import jax.numpy as jnp
from jax import lax
from jax.experimental import pallas as pl
from jax.experimental.pallas import tpu as pltpu
from jax.sharding import PartitionSpec as P

NORM_EPS = 1e-5
MESH = pl.DeviceIdType.MESH
LOG2E = 1.4426950408889634
LN2 = 0.6931471805599453
LOW = -1e30
CHUNK = 1024
SLOTS = 6
OTHER = 64
PAIRED = True
OWN_CHUNKS = 4


def kernel(
    tp_size, n_own, n_all, last_rows, first_rows, share_rows,
    hidden_hbm, draft_ref, temp_ref, gain_hbm, w_hbm,
    lp_ref, lse_ref, ent_ref,
    hv, gv, gs, gr, g2, buf, zs, vecs, ids_v, vecs_r, stats, msg, inbox,
    in_sem, w_sem, k_sem, g_send, g_recv, p_send, p_recv, f_send, f_recv, s_send, s_recv,
):
    dp, tp = lax.axis_index("dp"), lax.axis_index("tp")
    half = lax.rem(dp, 2)
    mate = dp + 1 - 2 * half
    core = lax.rem(tp, 2)
    twin = tp + 1 - 2 * core
    shard_rows, dim = w_hbm.shape
    batch, width = hidden_hbm.shape[:2]
    draft_len = draft_ref.shape[1]
    hd = dim // 2
    pad_rows = gs.shape[1]

    def peer(o, other):
        return (mate if other else dp, lax.rem(tp + o, tp_size))

    peers = [(o, False) for o in range(1, tp_size)]
    if PAIRED:
        peers += [(o, True) for o in range(tp_size)]

    barrier = pltpu.get_barrier_semaphore()
    for o, other in peers:
        pl.semaphore_signal(barrier, inc=1, device_id=peer(o, other), device_id_type=MESH)

    h_copy = pltpu.make_async_copy(hidden_hbm, hv, in_sem.at[0])
    gain_copy = pltpu.make_async_copy(gain_hbm, gv, in_sem.at[1])
    h_copy.start()
    gain_copy.start()

    own_rows = first_rows + n_own * CHUNK
    shared_base = own_rows + half * share_rows if PAIRED else own_rows

    def offset(j, late):
        if late:
            return shared_base + (j - 1 - n_own) * CHUNK
        return first_rows + (j - 1) * CHUNK

    def w_copy(j, late, rows=CHUNK):
        row = pl.multiple_of(offset(j, late), 16)
        slot = lax.rem(j, SLOTS)
        return pltpu.make_async_copy(w_hbm.at[pl.ds(row, rows)], buf.at[slot, pl.ds(0, rows)], w_sem.at[slot])

    def start_last():
        j = n_all - 1
        row = pl.multiple_of(offset(j, True), 16)
        for k in range(k_parts):
            last_copy(row, k).start()

    k_parts = k_sem.shape[0]
    k_width = dim // k_parts

    def last_copy(row, k):
        return pltpu.make_async_copy(
            w_hbm.at[pl.ds(row, last_rows), pl.ds(k * k_width, k_width)],
            buf.at[(n_all - 1) % SLOTS, pl.ds(0, last_rows), pl.ds(k * k_width, k_width)],
            k_sem.at[k],
        )

    first_copy = pltpu.make_async_copy(w_hbm.at[pl.ds(0, first_rows)], buf.at[0, pl.ds(0, first_rows)], w_sem.at[0])
    first_copy.start()
    for j in range(1, SLOTS):
        w_copy(j, j > n_own).start()

    lane = lax.broadcasted_iota(jnp.int32, (1, 128), 1)
    scale = jnp.zeros((1, 128), jnp.float32)
    ids = jnp.full((1, 128), -1, jnp.int32)
    for b in range(batch):
        inside = (lane >= b * width) & (lane < (b + 1) * width)
        scale = jnp.where(inside, temp_ref[b], scale)
        for i in range(draft_len):
            ids = jnp.where(lane == b * width + i, draft_ref[b, i], ids)
    scale = jnp.where(lane < batch * width, LOG2E / jnp.where(scale == 0.0, 1.0, scale), 0.0)
    vecs[...] = jnp.zeros_like(vecs)
    vecs[0:1, :] = scale
    vecs[1:2, :] = ids.astype(jnp.float32)
    ids_v[...] = jnp.broadcast_to(ids, (8, 128))
    stats[0] = jnp.full((8, 128), LOW, jnp.float32)
    stats[1] = jnp.zeros((8, 128), jnp.float32)
    stats[2] = jnp.zeros((8, 128), jnp.float32)
    stats[3] = jnp.zeros((8, 128), jnp.float32)
    g2[...] = jnp.zeros_like(g2)

    h_copy.wait()
    gain_copy.wait()
    gain = gv[...].astype(jnp.float32)
    for c in range(2):
        gs[c, batch * width :, :] = jnp.zeros((pad_rows - batch * width, hd), jnp.float32)
    for b in range(batch):
        hb = hv[b].astype(jnp.float32)
        mean_sq = jnp.sum(hb * hb, axis=-1, keepdims=True) * (1.0 / dim)
        g = (hb * lax.rsqrt(mean_sq + NORM_EPS) * gain).astype(jnp.bfloat16).astype(jnp.float32)
        for c in range(2):
            gs[c, b * width : (b + 1) * width, :] = g[:, c * hd : (c + 1) * hd]
    for c in range(2):
        g2[0:pad_rows, c * hd : (c + 1) * hd] = gs[c].astype(jnp.bfloat16)

    pl.semaphore_wait(barrier, len(peers))

    g_copy = pltpu.make_async_remote_copy(
        src_ref=gs.at[core], dst_ref=gr.at[core], send_sem=g_send, recv_sem=g_recv,
        device_id=(mate, tp), device_id_type=MESH)
    p_copy = pltpu.make_async_remote_copy(
        src_ref=vecs, dst_ref=vecs_r, send_sem=p_send, recv_sem=p_recv,
        device_id=(mate, tp), device_id_type=MESH)
    f_copy = pltpu.make_async_remote_copy(
        src_ref=gr.at[core], dst_ref=gr.at[core], send_sem=f_send, recv_sem=f_recv.at[core],
        device_id=(dp, twin), device_id_type=MESH)
    f_wait = pltpu.make_async_remote_copy(
        src_ref=gr.at[1 - core], dst_ref=gr.at[1 - core], send_sem=f_send, recv_sem=f_recv.at[1 - core],
        device_id=(dp, twin), device_id_type=MESH)
    if PAIRED:
        g_copy.start()
        p_copy.start()

    def forward():
        g_copy.wait_recv()
        f_copy.start()

    def join():
        f_wait.wait_recv()
        for c in range(2):
            g2[OTHER : OTHER + pad_rows, c * hd : (c + 1) * hd] = gr[c].astype(jnp.bfloat16)

    def join_lanes():
        p_copy.wait_recv()
        theirs = lane >= OTHER
        v = pltpu.roll(vecs_r[...], OTHER, 1)
        scale_all[...] = jnp.where(theirs, v[0:1], scale_all[...])
        ids_v[...] = jnp.where(theirs, jnp.broadcast_to(v[1:2].astype(jnp.int32), (8, 128)), ids_v[...])
        stats[0] = jnp.where(theirs, LOW, stats[0])
        for r in range(1, 4):
            stats[r] = jnp.where(theirs, 0.0, stats[r])

    scale_all = msg.at[1]
    scale_all[...] = jnp.broadcast_to(scale, (8, 128))

    def epilogue(z, base):
        rows = z.shape[0]
        z = z.reshape(rows // 8, 8, 128) * scale_all[...][None]
        old = stats[0]
        new = jnp.maximum(old, jnp.max(z, axis=0))
        e = jnp.exp2(z - new[None])
        fix = jnp.exp2(old - new)
        stats[0] = new
        stats[1] = stats[1] * fix + jnp.sum(e, axis=0)
        stats[2] = stats[2] * fix + jnp.sum(e * z, axis=0)
        row = lax.broadcasted_iota(jnp.int32, z.shape, 0) * 8 + lax.broadcasted_iota(jnp.int32, z.shape, 1)
        hit = row == (ids_v[...] - (tp * shard_rows + base))[None]
        stats[3] = stats[3] + jnp.sum(jnp.where(hit, z, 0.0), axis=0)

    def product(slot, rows, k0=0, k1=dim):
        part = rows // 2
        return [
            lax.dot_general(
                buf[slot, q * part : (q + 1) * part, k0:k1], g2[:, k0:k1],
                (((1,), (1,)), ((), ())), preferred_element_type=jnp.float32)
            for q in range(2)
        ]

    def put(par, parts):
        rows = parts[0].shape[0]
        for q in range(2):
            zs[par, q * rows : (q + 1) * rows] = parts[q]

    def drain(par, base):
        part = CHUNK // 2
        for q in range(2):
            epilogue(zs[par, q * part : (q + 1) * part], base + q * part)

    def start_chunk(j):
        if j < n_all - 1:
            w_copy(jnp.int32(j), True).start()
        elif j == n_all - 1:
            start_last()

    first_copy.wait()
    parts = product(0, first_rows)
    start_chunk(SLOTS)
    for q in range(2):
        epilogue(parts[q], q * (first_rows // 2))

    late0 = n_own + 1
    forward_at = late0 - 1

    def base_of(j):
        early = first_rows + (j - 1) * CHUNK
        return early + jnp.where(j >= late0, shared_base - own_rows, 0)

    def step(j, par):
        slot = lax.rem(j, SLOTS)
        if PAIRED and forward_at % 2 == par:
            pl.when(j == forward_at)(forward)
        if PAIRED and late0 % 2 == par:
            pl.when(j == late0)(join)
        pltpu.make_async_copy(w_hbm.at[pl.ds(0, CHUNK)], buf.at[slot], w_sem.at[slot]).wait()
        parts = product(slot, CHUNK)

        if isinstance(j, int):
            put(par, parts)
            start_chunk(j + SLOTS)
            return
        drain(1 - par, base_of(j - 1))
        put(par, parts)
        if PAIRED and late0 % 2 == par:
            pl.when(j == late0)(join_lanes)

        @pl.when(j + SLOTS < n_all - 1)
        def _():
            w_copy(j + SLOTS, True).start()

        @pl.when(j + SLOTS == n_all - 1)
        def _():
            start_last()

    step(1, 1)
    n_loop = n_all - 3

    def body(i, carry):
        step(2 + 2 * i, 0)
        step(3 + 2 * i, 1)
        return carry

    lax.fori_loop(0, n_loop // 2, body, 0)
    if n_loop % 2:
        step(jnp.int32(n_all - 2), 0)

    row = pl.multiple_of(offset(n_all - 1, True), 16)
    parts = None
    for k in range(k_parts):
        last_copy(row, k).wait()
        more = product((n_all - 1) % SLOTS, last_rows, k * k_width, (k + 1) * k_width)
        parts = more if parts is None else [x + y for x, y in zip(parts, more)]
        if k == 0:
            drain((n_all - 2) % 2, base_of(n_all - 2))
    for q in range(2):
        epilogue(parts[q], row + q * (last_rows // 2))

    m8 = stats[0]
    m1 = jnp.max(m8, axis=0, keepdims=True)
    w8 = jnp.exp2(m8 - m1)
    out = msg.at[0]
    out[4:8, :] = jnp.zeros((4, 128), jnp.float32)
    out[0:1, :] = m1
    out[1:2, :] = jnp.sum(stats[1] * w8, axis=0, keepdims=True)
    out[2:3, :] = jnp.sum(stats[2] * w8, axis=0, keepdims=True)
    out[3:4, :] = jnp.sum(stats[3], axis=0, keepdims=True)

    def s_copy(o, other, source):
        i = 1 if other else 0
        return pltpu.make_async_remote_copy(
            src_ref=msg.at[0], dst_ref=inbox.at[i, source], send_sem=s_send.at[i, o], recv_sem=s_recv.at[i, source],
            device_id=peer(o, other), device_id_type=MESH)

    for o, other in peers:
        s_copy(o, other, tp).start()
    inbox[0, tp] = msg[0]
    for o, other in peers:
        s_copy(o, other, lax.rem(tp - o + tp_size, tp_size)).wait_recv()

    def combine(x):
        m = jnp.max(x[:, 0:1, :], axis=0)
        r = lax.broadcasted_iota(jnp.int32, x.shape, 1)
        weight = jnp.exp2(x[:, 0:1, :] - m[None])
        s = jnp.sum(jnp.where((r == 1) | (r == 2), x * weight, x), axis=0)
        return m, s

    m, s = combine(inbox[0])
    if PAIRED:
        m2, s2 = combine(inbox[1])
        m2 = pltpu.roll(jnp.broadcast_to(m2, (8, 128)), OTHER, 1)[0:1]
        s2 = pltpu.roll(s2, OTHER, 1)
        top = jnp.maximum(m, m2)
        r = lax.broadcasted_iota(jnp.int32, s.shape, 0)
        ours, theirs = jnp.exp2(m - top), jnp.exp2(m2 - top)
        scaled = (r == 1) | (r == 2)
        s = jnp.where(scaled, s * ours, s) + jnp.where(scaled, s2 * theirs, s2)
        m = top
    lse = m * LN2 + jnp.log(s[1:2])
    ent = lse - LN2 * (s[2:3] / s[1:2])
    lp = LN2 * s[3:4] - lse

    if PAIRED:
        p_copy.wait_send()
    vecs[0:1, :] = lse
    vecs[1:2, :] = ent
    vecs[2:3, :] = lp
    for b in range(batch):
        line = pltpu.roll(vecs[...], (128 - b * width) % 128, 1)
        lse_ref[b : b + 1, :] = line[0:1, :width]
        ent_ref[b : b + 1, :] = line[1:2, :width]
        lp_ref[b : b + 1, :] = line[2:3, :draft_len]

    for o, other in peers:
        s_copy(o, other, tp).wait_send()
    if PAIRED:
        g_copy.wait_send()
        f_copy.wait_send()


def solution(mesh):
    tp_size = mesh.shape["tp"]

    def local_step(hidden, draft_ids, temperature, norm_gain, head_shard):
        batch, width, dim = hidden.shape
        shard_rows = head_shard.shape[0]
        first_rows = shard_rows % CHUNK
        full = shard_rows // CHUNK
        if PAIRED:
            n_own = OWN_CHUNKS
            share_rows = (shard_rows - first_rows - n_own * CHUNK) // 2
            n_late = -(-share_rows // CHUNK)
            last_rows = share_rows - (n_late - 1) * CHUNK
            n_all = 1 + n_own + n_late
        else:
            n_own, share_rows, n_all, last_rows = 0, 0, 1 + full, CHUNK
        pad_rows = -(-batch * width // 8) * 8
        vmem, dma = pltpu.VMEM, pltpu.SemaphoreType.DMA
        f32, bf16 = jnp.float32, jnp.bfloat16
        any_space = pl.BlockSpec(memory_space=pltpu.HBM)
        smem = pl.BlockSpec(memory_space=pltpu.SMEM)
        out = pl.BlockSpec(memory_space=pltpu.VMEM)
        return pl.pallas_call(
            functools.partial(kernel, tp_size, n_own, n_all, last_rows, first_rows, share_rows),
            out_shape=(
                jax.ShapeDtypeStruct(draft_ids.shape, f32),
                jax.ShapeDtypeStruct((batch, width), f32),
                jax.ShapeDtypeStruct((batch, width), f32),
            ),
            in_specs=[any_space, smem, smem, any_space, any_space],
            out_specs=(out, out, out),
            scratch_shapes=[
                vmem(hidden.shape, bf16),
                vmem((1, dim), bf16),
                vmem((2, pad_rows, dim // 2), f32),
                vmem((2, pad_rows, dim // 2), f32),
                vmem((128, dim), bf16),
                vmem((SLOTS, CHUNK, dim), bf16),
                vmem((2, CHUNK, 128), f32),
                vmem((8, 128), f32),
                vmem((8, 128), jnp.int32),
                vmem((8, 128), f32),
                vmem((4, 8, 128), f32),
                vmem((2, 8, 128), f32),
                vmem((2, tp_size, 8, 128), f32),
                dma((2,)), dma((SLOTS,)), dma((4,)),
                dma, dma, dma, dma, dma, dma((2,)),
                dma((2, tp_size)), dma((2, tp_size)),
            ],
            compiler_params=pltpu.CompilerParams(
                collective_id=0, has_side_effects=True, vmem_limit_bytes=60 * 2**20),
        )(hidden, draft_ids, temperature, norm_gain.reshape(1, dim), head_shard)

    return jax.shard_map(
        local_step,
        mesh=mesh,
        in_specs=(P("dp", None, None), P("dp", None), P("dp"), P(None), P("tp", None)),
        out_specs=(P("dp", None), P("dp", None), P("dp", None)),
        check_vma=False,
    )
```

```python
import functools

import jax
import jax.numpy as jnp
from jax import lax
from jax.experimental import pallas as pl
from jax.experimental.pallas import tpu as pltpu
from jax.sharding import PartitionSpec as P

NORM_EPS = 1e-5
MESH = pl.DeviceIdType.MESH
LOG2E = 1.4426950408889634
LN2 = 0.6931471805599453
LOW = -1e30
CHUNK = 1024
SLOTS = 6
OTHER = 64
PAIRED = True
OWN_CHUNKS = 4


def kernel(
    tp_size, n_own, n_all, last_rows, first_rows, share_rows,
    hidden_hbm, draft_hbm, temp_hbm, gain_hbm, w_hbm,
    out_ref,
    draft_ref, temp_ref, hv, gv, gs, gr, g2, buf, zs, vecs, ids_v, vecs_r, stats, msg, inbox,
    in_sem, w_sem, k_sem, g_send, g_recv, p_send, p_recv, f_send, f_recv, s_send, s_recv,
):
    dp, tp = lax.axis_index("dp"), lax.axis_index("tp")
    half = lax.rem(dp, 2)
    mate = dp + 1 - 2 * half
    core = lax.rem(tp, 2)
    twin = tp + 1 - 2 * core
    shard_rows, dim = w_hbm.shape
    batch, width = hidden_hbm.shape[:2]
    draft_len = draft_hbm.shape[1]
    hd = dim // 2
    pad_rows = gs.shape[1]

    def peer(o, other):
        return (mate if other else dp, lax.rem(tp + o, tp_size))

    far_first = sorted(range(tp_size), key=lambda o: -min(o, tp_size - o))
    peers = [(o, True) for o in far_first] if PAIRED else []
    peers += [(o, False) for o in far_first if o]

    barrier = pltpu.get_barrier_semaphore()
    for o, other in peers:
        pl.semaphore_signal(barrier, inc=1, device_id=peer(o, other), device_id_type=MESH)

    h_copy = pltpu.make_async_copy(hidden_hbm, hv, in_sem.at[0])
    gain_copy = pltpu.make_async_copy(gain_hbm, gv, in_sem.at[1])
    draft_copy = pltpu.make_async_copy(draft_hbm, draft_ref, in_sem.at[2])
    temp_copy = pltpu.make_async_copy(temp_hbm, temp_ref, in_sem.at[3])
    h_copy.start()
    gain_copy.start()
    draft_copy.start()
    temp_copy.start()

    own_rows = first_rows + n_own * CHUNK
    shared_base = own_rows + half * share_rows if PAIRED else own_rows

    def offset(j, late):
        if late:
            return shared_base + (j - 1 - n_own) * CHUNK
        return first_rows + (j - 1) * CHUNK

    def w_copy(j, late, rows=CHUNK):
        row = pl.multiple_of(offset(j, late), 16)
        slot = lax.rem(j, SLOTS)
        return pltpu.make_async_copy(w_hbm.at[pl.ds(row, rows)], buf.at[slot, pl.ds(0, rows)], w_sem.at[slot])

    def start_last():
        j = n_all - 1
        row = pl.multiple_of(offset(j, True), 16)
        for k in range(k_parts):
            last_copy(row, k).start(priority=1)

    k_parts = k_sem.shape[0]
    k_width = dim // k_parts

    def last_copy(row, k):
        return pltpu.make_async_copy(
            w_hbm.at[pl.ds(row, last_rows), pl.ds(k * k_width, k_width)],
            buf.at[(n_all - 1) % SLOTS, pl.ds(0, last_rows), pl.ds(k * k_width, k_width)],
            k_sem.at[k],
        )

    first_copy = pltpu.make_async_copy(w_hbm.at[pl.ds(0, first_rows)], buf.at[0, pl.ds(0, first_rows)], w_sem.at[0])
    first_copy.start(priority=1)
    for j in range(1, SLOTS):
        w_copy(j, j > n_own).start(priority=1)

    draft_copy.wait()
    temp_copy.wait()
    lane = lax.broadcasted_iota(jnp.int32, (1, 128), 1)
    scale = jnp.zeros((1, 128), jnp.float32)
    ids = jnp.full((1, 128), -1, jnp.int32)
    for b in range(batch):
        inside = (lane >= b * width) & (lane < (b + 1) * width)
        scale = jnp.where(inside, temp_ref[b], scale)
        for i in range(draft_len):
            ids = jnp.where(lane == b * width + i, draft_ref[b, i], ids)
    scale = jnp.where(lane < batch * width, LOG2E / jnp.where(scale == 0.0, 1.0, scale), 0.0)
    vecs[...] = jnp.zeros_like(vecs)
    vecs[0:1, :] = scale
    vecs[1:2, :] = ids.astype(jnp.float32)
    ids_v[...] = jnp.broadcast_to(ids, (8, 128))
    stats[0] = jnp.full((8, 128), LOW, jnp.float32)
    stats[1] = jnp.zeros((8, 128), jnp.float32)
    stats[2] = jnp.zeros((8, 128), jnp.float32)
    stats[3] = jnp.zeros((8, 128), jnp.float32)
    g2[...] = jnp.zeros_like(g2)

    h_copy.wait()
    gain_copy.wait()
    gain = gv[...].astype(jnp.float32).reshape(1, dim)
    for c in range(2):
        gs[c, batch * width :, :] = jnp.zeros((pad_rows - batch * width, hd), jnp.float32)
    for b in range(batch):
        hb = hv[b].astype(jnp.float32)
        mean_sq = jnp.sum(hb * hb, axis=-1, keepdims=True) * (1.0 / dim)
        g = (hb * lax.rsqrt(mean_sq + NORM_EPS) * gain).astype(jnp.bfloat16).astype(jnp.float32)
        for c in range(2):
            gs[c, b * width : (b + 1) * width, :] = g[:, c * hd : (c + 1) * hd]
    for c in range(2):
        g2[0:pad_rows, c * hd : (c + 1) * hd] = gs[c].astype(jnp.bfloat16)

    g_copy = pltpu.make_async_remote_copy(
        src_ref=gs.at[core], dst_ref=gr.at[core], send_sem=g_send, recv_sem=g_recv,
        device_id=(mate, tp), device_id_type=MESH)
    p_copy = pltpu.make_async_remote_copy(
        src_ref=vecs, dst_ref=vecs_r, send_sem=p_send, recv_sem=p_recv,
        device_id=(mate, tp), device_id_type=MESH)
    f_copy = pltpu.make_async_remote_copy(
        src_ref=gr.at[core], dst_ref=gr.at[core], send_sem=f_send, recv_sem=f_recv.at[core],
        device_id=(dp, twin), device_id_type=MESH)
    f_wait = pltpu.make_async_remote_copy(
        src_ref=gr.at[1 - core], dst_ref=gr.at[1 - core], send_sem=f_send, recv_sem=f_recv.at[1 - core],
        device_id=(dp, twin), device_id_type=MESH)
    def forward():
        g_copy.wait_recv()
        f_copy.start()

    def join():
        f_wait.wait_recv()
        for c in range(2):
            g2[OTHER : OTHER + pad_rows, c * hd : (c + 1) * hd] = gr[c].astype(jnp.bfloat16)

    def join_lanes():
        p_copy.wait_recv()
        theirs = lane >= OTHER
        v = pltpu.roll(vecs_r[...], OTHER, 1)
        scale_all[...] = jnp.where(theirs, v[0:1], scale_all[...])
        ids_v[...] = jnp.where(theirs, jnp.broadcast_to(v[1:2].astype(jnp.int32), (8, 128)), ids_v[...])
        stats[0] = jnp.where(theirs, LOW, stats[0])
        for r in range(1, 4):
            stats[r] = jnp.where(theirs, 0.0, stats[r])

    scale_all = msg.at[1]
    scale_all[...] = jnp.broadcast_to(scale, (8, 128))

    def epilogue(z, base):
        rows = z.shape[0]
        z = z.reshape(rows // 8, 8, 128) * scale_all[...][None]
        old = stats[0]
        new = jnp.maximum(old, jnp.max(z, axis=0))
        e = jnp.exp2(z - new[None])
        fix = jnp.exp2(old - new)
        stats[0] = new
        stats[1] = stats[1] * fix + jnp.sum(e, axis=0)
        stats[2] = stats[2] * fix + jnp.sum(e * z, axis=0)
        row = lax.broadcasted_iota(jnp.int32, z.shape, 0) * 8 + lax.broadcasted_iota(jnp.int32, z.shape, 1)
        hit = row == (ids_v[...] - (tp * shard_rows + base))[None]
        stats[3] = stats[3] + jnp.sum(jnp.where(hit, z, 0.0), axis=0)

    def product(slot, rows, k0=0, k1=dim):
        part = rows // 2
        return [
            lax.dot_general(
                buf[slot, q * part : (q + 1) * part, k0:k1], g2[:, k0:k1],
                (((1,), (1,)), ((), ())), preferred_element_type=jnp.float32)
            for q in range(2)
        ]

    def put(par, parts):
        rows = parts[0].shape[0]
        for q in range(2):
            zs[par, q * rows : (q + 1) * rows] = parts[q]

    def drain(par, base):
        part = CHUNK // 2
        for q in range(2):
            epilogue(zs[par, q * part : (q + 1) * part], base + q * part)

    def start_chunk(j):
        if j < n_all - 1:
            w_copy(jnp.int32(j), True).start(priority=1)
        elif j == n_all - 1:
            start_last()

    first_copy.wait()
    pl.semaphore_wait(barrier, len(peers))
    if PAIRED:
        g_copy.start()
        p_copy.start()
    parts = product(0, first_rows)
    start_chunk(SLOTS)
    for q in range(2):
        epilogue(parts[q], q * (first_rows // 2))

    late0 = n_own + 1
    forward_at = late0 - 1

    def base_of(j):
        early = first_rows + (j - 1) * CHUNK
        return early + jnp.where(j >= late0, shared_base - own_rows, 0)

    def step(j, par):
        slot = lax.rem(j, SLOTS)
        if PAIRED and forward_at % 2 == par:
            pl.when(j == forward_at)(forward)
        if PAIRED and late0 % 2 == par:
            pl.when(j == late0)(join)
        pltpu.make_async_copy(w_hbm.at[pl.ds(0, CHUNK)], buf.at[slot], w_sem.at[slot]).wait()
        parts = product(slot, CHUNK)

        if isinstance(j, int):
            put(par, parts)
            start_chunk(j + SLOTS)
            return
        drain(1 - par, base_of(j - 1))
        put(par, parts)
        if PAIRED and late0 % 2 == par:
            pl.when(j == late0)(join_lanes)

        @pl.when(j + SLOTS < n_all - 1)
        def _():
            w_copy(j + SLOTS, True).start(priority=1)

        @pl.when(j + SLOTS == n_all - 1)
        def _():
            start_last()

    step(1, 1)
    n_loop = n_all - 3

    def body(i, carry):
        step(2 + 2 * i, 0)
        step(3 + 2 * i, 1)
        return carry

    lax.fori_loop(0, n_loop // 2, body, 0)
    if n_loop % 2:
        step(jnp.int32(n_all - 2), 0)

    row = pl.multiple_of(offset(n_all - 1, True), 16)
    parts = None
    for k in range(k_parts):
        last_copy(row, k).wait()
        more = product((n_all - 1) % SLOTS, last_rows, k * k_width, (k + 1) * k_width)
        parts = more if parts is None else [x + y for x, y in zip(parts, more)]
        if k == 0:
            drain((n_all - 2) % 2, base_of(n_all - 2))
    for q in range(2):
        epilogue(parts[q], row + q * (last_rows // 2))

    m8 = stats[0]
    m1 = jnp.max(m8, axis=0, keepdims=True)
    w8 = jnp.exp2(m8 - m1)
    out = msg.at[0]
    out[4:8, :] = jnp.zeros((4, 128), jnp.float32)
    out[0:1, :] = m1
    out[1:2, :] = jnp.sum(stats[1] * w8, axis=0, keepdims=True)
    out[2:3, :] = jnp.sum(stats[2] * w8, axis=0, keepdims=True)
    out[3:4, :] = jnp.sum(stats[3], axis=0, keepdims=True)

    def s_copy(o, other, source):
        i = 1 if other else 0
        return pltpu.make_async_remote_copy(
            src_ref=msg.at[0], dst_ref=inbox.at[i, source], send_sem=s_send.at[i, o], recv_sem=s_recv.at[i, source],
            device_id=peer(o, other), device_id_type=MESH)

    for o, other in peers:
        s_copy(o, other, tp).start()
    inbox[0, tp] = msg[0]
    for o, other in peers:
        s_copy(o, other, lax.rem(tp - o + tp_size, tp_size)).wait_recv()

    def combine(x):
        m = jnp.max(x[:, 0:1, :], axis=0)
        r = lax.broadcasted_iota(jnp.int32, x.shape, 1)
        weight = jnp.exp2(x[:, 0:1, :] - m[None])
        s = jnp.sum(jnp.where((r == 1) | (r == 2), x * weight, x), axis=0)
        return m, s

    m, s = combine(inbox[0])
    if PAIRED:
        m2, s2 = combine(inbox[1])
        m2 = pltpu.roll(jnp.broadcast_to(m2, (8, 128)), OTHER, 1)[0:1]
        s2 = pltpu.roll(s2, OTHER, 1)
        top = jnp.maximum(m, m2)
        r = lax.broadcasted_iota(jnp.int32, s.shape, 0)
        ours, theirs = jnp.exp2(m - top), jnp.exp2(m2 - top)
        scaled = (r == 1) | (r == 2)
        s = jnp.where(scaled, s * ours, s) + jnp.where(scaled, s2 * theirs, s2)
        m = top
    lse = m * LN2 + jnp.log(s[1:2])
    ent = lse - LN2 * (s[2:3] / s[1:2])
    lp = LN2 * s[3:4] - lse

    if PAIRED:
        p_copy.wait_send()
    vecs[0:1, :] = lse
    vecs[1:2, :] = ent
    vecs[2:3, :] = lp
    out_ref[...] = vecs[...]

    for o, other in peers:
        s_copy(o, other, tp).wait_send()
    if PAIRED:
        g_copy.wait_send()
        f_copy.wait_send()


def unpack(lines_ref, lp_ref, lse_ref, ent_ref):
    batch, width = lse_ref.shape
    for b in range(batch):
        line = pltpu.roll(lines_ref[...], (128 - b * width) % 128, 1)
        lse_ref[b : b + 1, :] = line[0:1, :width]
        ent_ref[b : b + 1, :] = line[1:2, :width]
        lp_ref[b : b + 1, :] = line[2:3, : lp_ref.shape[1]]


def solution(mesh):
    tp_size = mesh.shape["tp"]

    def local_step(hidden, draft_ids, temperature, norm_gain, head_shard):
        batch, width, dim = hidden.shape
        shard_rows = head_shard.shape[0]
        first_rows = shard_rows % CHUNK
        full = shard_rows // CHUNK
        if PAIRED:
            n_own = OWN_CHUNKS
            share_rows = (shard_rows - first_rows - n_own * CHUNK) // 2
            n_late = -(-share_rows // CHUNK)
            last_rows = share_rows - (n_late - 1) * CHUNK
            n_all = 1 + n_own + n_late
        else:
            n_own, share_rows, n_all, last_rows = 0, 0, 1 + full, CHUNK
        pad_rows = -(-batch * width // 8) * 8
        vmem, dma = pltpu.VMEM, pltpu.SemaphoreType.DMA
        f32, bf16 = jnp.float32, jnp.bfloat16
        any_space = pl.BlockSpec(memory_space=pltpu.HBM)
        out = pl.BlockSpec(memory_space=pltpu.VMEM)
        lines = pl.pallas_call(
            functools.partial(kernel, tp_size, n_own, n_all, last_rows, first_rows, share_rows),
            out_shape=pltpu.VMEM((8, 128), f32),
            in_specs=[any_space] * 5,
            out_specs=out,
            scratch_shapes=[
                pltpu.SMEM(draft_ids.shape, jnp.int32),
                pltpu.SMEM(temperature.shape, f32),
                vmem(hidden.shape, bf16),
                vmem((dim,), bf16),
                vmem((2, pad_rows, dim // 2), f32),
                vmem((2, pad_rows, dim // 2), f32),
                vmem((128, dim), bf16),
                vmem((SLOTS, CHUNK, dim), bf16),
                vmem((2, CHUNK, 128), f32),
                vmem((8, 128), f32),
                vmem((8, 128), jnp.int32),
                vmem((8, 128), f32),
                vmem((4, 8, 128), f32),
                vmem((2, 8, 128), f32),
                vmem((2, tp_size, 8, 128), f32),
                dma((4,)), dma((SLOTS,)), dma((1,)),
                dma, dma, dma, dma, dma, dma((2,)),
                dma((2, tp_size)), dma((2, tp_size)),
            ],
            compiler_params=pltpu.CompilerParams(
                collective_id=0, has_side_effects=True, vmem_limit_bytes=60 * 2**20),
        )(hidden, draft_ids, temperature, norm_gain, head_shard)
        return pl.pallas_call(
            unpack,
            out_shape=(
                jax.ShapeDtypeStruct(draft_ids.shape, f32),
                jax.ShapeDtypeStruct((batch, width), f32),
                jax.ShapeDtypeStruct((batch, width), f32),
            ),
            in_specs=[out],
            out_specs=(out, out, out),
        )(pltpu.with_memory_space_constraint(lines, pltpu.VMEM))

    return jax.shard_map(
        local_step,
        mesh=mesh,
        in_specs=(P("dp", None, None), P("dp", None), P("dp"), P(None), P("tp", None)),
        out_specs=(P("dp", None), P("dp", None), P("dp", None)),
        check_vma=False,
    )
```

```python
import functools

import jax
import jax.numpy as jnp
from jax import lax
from jax.experimental import pallas as pl
from jax.experimental.pallas import tpu as pltpu
from jax.sharding import PartitionSpec as P

NORM_EPS = 1e-5
MESH = pl.DeviceIdType.MESH
LOG2E = 1.4426950408889634
LN2 = 0.6931471805599453
LOW = -1e30
CHUNK = 1024
SLOTS = 6
OTHER = 64
PAIRED = True
BLOCKS_OWN = [[2], [3], [4]]
BLOCKS_LATE = [[0], [1], [2], [3], [4], [5]]
OWN_CHUNKS = 3


def kernel(
    tp_size, blocks, n_own, n_all, last_rows, first_rows, share_rows,
    hidden_hbm, draft_hbm, temp_hbm, gain_hbm, w_hbm,
    out_ref,
    draft_ref, temp_ref, hv, gv, gs, gr, g2, buf, zs, vecs, ids_v, vecs_r, stats, msg, inbox,
    in_sem, w_sem, g_send, g_recv, p_send, p_recv, f_send, f_recv, s_send, s_recv,
):
    dp, tp = lax.axis_index("dp"), lax.axis_index("tp")
    half = lax.rem(dp, 2)
    mate = dp + 1 - 2 * half
    core = lax.rem(tp, 2)
    twin = tp + 1 - 2 * core
    shard_rows, dim = w_hbm.shape
    batch, width = hidden_hbm.shape[:2]
    draft_len = draft_hbm.shape[1]
    hd = dim // 2

    def peer(o, other):
        return (mate if other else dp, lax.rem(tp + o, tp_size))

    far_first = sorted(range(tp_size), key=lambda o: -min(o, tp_size - o))
    peers = [(o, True) for o in far_first] if PAIRED else []
    peers += [(o, False) for o in far_first if o]

    own_rows = first_rows[0] + first_rows[1] + n_own * CHUNK
    shared_base = own_rows + half * share_rows if PAIRED else own_rows

    def chunk(j):
        if j == 0:
            return 0, first_rows[0], 0, 0
        if j == 1:
            return first_rows[0], first_rows[1], 0, first_rows[0]
        rows = last_rows if j == n_all - 1 else CHUNK
        early = first_rows[0] + first_rows[1] + (j - 2) * CHUNK
        if j - 2 < n_own:
            return early, rows, (j - 1) % SLOTS, 0
        return shared_base + (j - 2 - n_own) * CHUNK, rows, (j - 1) % SLOTS, 0

    def w_copy(j):
        row, rows, slot, at = chunk(j)
        if not isinstance(row, int):
            row = pl.multiple_of(row, 16)
        return pltpu.make_async_copy(
            w_hbm.at[pl.ds(row, rows)], buf.at[slot, pl.ds(at, rows)], w_sem.at[0 if j == 0 else slot + 1])

    h_copy = pltpu.make_async_copy(hidden_hbm, hv, in_sem.at[0])
    gain_copy = pltpu.make_async_copy(gain_hbm, gv, in_sem.at[1])
    draft_copy = pltpu.make_async_copy(draft_hbm, draft_ref, in_sem.at[2])
    temp_copy = pltpu.make_async_copy(temp_hbm, temp_ref, in_sem.at[3])
    h_copy.start()
    gain_copy.start()
    draft_copy.start()
    temp_copy.start()
    for j in range(SLOTS + 1):
        w_copy(j).start(priority=1)

    barrier = pltpu.get_barrier_semaphore()
    for o, other in peers:
        pl.semaphore_signal(barrier, inc=1, device_id=peer(o, other), device_id_type=MESH)

    draft_copy.wait()
    temp_copy.wait()
    lane = lax.broadcasted_iota(jnp.int32, (1, 128), 1)
    scale = jnp.zeros((1, 128), jnp.float32)
    ids = jnp.full((1, 128), -1, jnp.int32)
    for b in range(batch):
        inside = (lane >= b * width) & (lane < (b + 1) * width)
        scale = jnp.where(inside, temp_ref[b], scale)
        for i in range(draft_len):
            ids = jnp.where(lane == b * width + i, draft_ref[b, i], ids)
    scale = jnp.where(lane < batch * width, LOG2E / jnp.where(scale == 0.0, 1.0, scale), 0.0)
    vecs[...] = jnp.zeros_like(vecs)
    vecs[0:1, :] = scale
    vecs[1:2, :] = ids.astype(jnp.float32)
    ids_v[...] = jnp.broadcast_to(ids, (8, 128))
    stats[0] = jnp.full((8, 128), LOW, jnp.float32)
    stats[1] = jnp.zeros((8, 128), jnp.float32)
    stats[2] = jnp.zeros((8, 128), jnp.float32)
    stats[3] = jnp.zeros((8, 128), jnp.float32)
    g2[...] = jnp.zeros_like(g2)

    h_copy.wait()
    gain_copy.wait()
    gain = gv[...].astype(jnp.float32).reshape(1, dim)
    n_pos, n_k = batch * width, hd // 128

    def place(src, h, row):
        for k in range(n_k):
            ks = pl.ds(pl.multiple_of(h * hd + k * 128, 128), 128)
            g2[row : row + n_pos, ks] = src[h, pl.ds(k, n_pos, stride=n_k), :].astype(jnp.bfloat16)

    for b in range(batch):
        hb = hv[b].astype(jnp.float32)
        mean_sq = jnp.sum(hb * hb, axis=-1, keepdims=True) * (1.0 / dim)
        g = (hb * lax.rsqrt(mean_sq + NORM_EPS) * gain).astype(jnp.bfloat16).astype(jnp.float32)
        for c in range(2):
            for k in range(n_k):
                at = c * hd + k * 128
                gs[c, pl.ds(b * width * n_k + k, width, stride=n_k), :] = g[:, at : at + 128]
    for c in range(2):
        place(gs, c, 0)

    g_copy = pltpu.make_async_remote_copy(
        src_ref=gs.at[core], dst_ref=gr.at[core], send_sem=g_send, recv_sem=g_recv,
        device_id=(mate, tp), device_id_type=MESH)
    p_copy = pltpu.make_async_remote_copy(
        src_ref=vecs, dst_ref=vecs_r, send_sem=p_send, recv_sem=p_recv,
        device_id=(mate, tp), device_id_type=MESH)
    f_copy = pltpu.make_async_remote_copy(
        src_ref=gr.at[core], dst_ref=gr.at[core], send_sem=f_send, recv_sem=f_recv.at[core],
        device_id=(dp, twin), device_id_type=MESH)
    f_wait = pltpu.make_async_remote_copy(
        src_ref=gr.at[1 - core], dst_ref=gr.at[1 - core], send_sem=f_send, recv_sem=f_recv.at[1 - core],
        device_id=(dp, twin), device_id_type=MESH)
    def forward():
        g_copy.wait_recv()
        f_copy.start()

    def join(h):
        place(gr, h, OTHER)

    def join_lanes():
        p_copy.wait_recv()
        theirs = lane >= OTHER
        v = pltpu.roll(vecs_r[...], OTHER, 1)
        scale_all[...] = jnp.where(theirs, v[0:1], scale_all[...])
        ids_v[...] = jnp.where(theirs, jnp.broadcast_to(v[1:2].astype(jnp.int32), (8, 128)), ids_v[...])
        stats[0] = jnp.where(theirs, LOW, stats[0])
        for r in range(1, 4):
            stats[r] = jnp.where(theirs, 0.0, stats[r])

    scale_all = msg.at[1]
    scale_all[...] = jnp.broadcast_to(scale, (8, 128))

    def epilogue(z, base):
        rows = z.shape[0]
        z = z.reshape(rows // 8, 8, 128) * scale_all[...][None]
        old = stats[0]
        new = jnp.maximum(old, jnp.max(z, axis=0))
        e = jnp.exp2(z - new[None])
        fix = jnp.exp2(old - new)
        stats[0] = new
        stats[1] = stats[1] * fix + jnp.sum(e, axis=0)
        stats[2] = stats[2] * fix + jnp.sum(e * z, axis=0)
        row = lax.broadcasted_iota(jnp.int32, z.shape, 0) * 8 + lax.broadcasted_iota(jnp.int32, z.shape, 1)
        hit = row == (ids_v[...] - (tp * shard_rows + base))[None]
        stats[3] = stats[3] + jnp.sum(jnp.where(hit, z, 0.0), axis=0)

    def product(j):
        _, rows, slot, at = chunk(j)
        part = rows // 2
        return [
            lax.dot_general(
                buf[slot, at + q * part : at + (q + 1) * part], g2[...],
                (((1,), (1,)), ((), ())), preferred_element_type=jnp.float32)
            for q in range(2)
        ]

    def half_product(j, h):
        _, rows, slot, at = chunk(j)
        part = rows // 2
        ks = pl.ds(pl.multiple_of(h * hd, 128), hd)
        return [
            lax.dot_general(
                buf[slot, pl.ds(at + q * part, part), ks], g2[:, ks],
                (((1,), (1,)), ((), ())), preferred_element_type=jnp.float32)
            for q in range(2)
        ]

    def drain(done):
        for j, z in done:
            base, rows = chunk(j)[:2]
            part = rows // 2
            for q in range(2):
                epilogue(zs[z, q * part : (q + 1) * part], base + q * part)

    done = []
    for n, block in enumerate(blocks):
        forwarding = PAIRED and block[0] == n_own + 1
        joining = PAIRED and block[0] == n_own + 2
        if joining:
            join(core)
        for j in block:
            w_copy(j).wait()
        if n == 0:
            pl.semaphore_wait(barrier, len(peers))
            if PAIRED:
                g_copy.start()
                p_copy.start()
        if forwarding or joining:
            first = half_product(block[0], core)
            if forwarding:
                z = 2 * (n % 2)
                for q in range(2):
                    zs[z, q * (CHUNK // 2) : (q + 1) * (CHUNK // 2)] = first[q]
                forward()
                second = half_product(block[0], 1 - core)
                first = [zs[z, q * (CHUNK // 2) : (q + 1) * (CHUNK // 2)] for q in range(2)]
            else:
                drain(done)
                done = []
                z = 2 * (n % 2)
                for q in range(2):
                    zs[z, q * (CHUNK // 2) : (q + 1) * (CHUNK // 2)] = first[q]
                f_wait.wait_recv()
                join(1 - core)
                second = half_product(block[0], 1 - core)
                first = [zs[z, q * (CHUNK // 2) : (q + 1) * (CHUNK // 2)] for q in range(2)]
            parts = [[x + y for x, y in zip(first, second)]]
        else:
            parts = [product(j) for j in block]
        drain(done)
        done = [(j, 2 * (n % 2) + i) for i, j in enumerate(block)]
        for (j, z), p in zip(done, parts):
            rows = p[0].shape[0]
            for q in range(2):
                zs[z, q * rows : (q + 1) * rows] = p[q]
        if joining:
            join_lanes()
        for j in block:
            if 1 <= j and j + SLOTS < n_all:
                w_copy(j + SLOTS).start(priority=1)
    drain(done)

    m8 = stats[0]
    m1 = jnp.max(m8, axis=0, keepdims=True)
    w8 = jnp.exp2(m8 - m1)
    out = msg.at[0]
    out[4:8, :] = jnp.zeros((4, 128), jnp.float32)
    out[0:1, :] = m1
    out[1:2, :] = jnp.sum(stats[1] * w8, axis=0, keepdims=True)
    out[2:3, :] = jnp.sum(stats[2] * w8, axis=0, keepdims=True)
    out[3:4, :] = jnp.sum(stats[3], axis=0, keepdims=True)

    def s_copy(o, other, source):
        i = 1 if other else 0
        return pltpu.make_async_remote_copy(
            src_ref=msg.at[0], dst_ref=inbox.at[i * tp_size + source], send_sem=s_send, recv_sem=s_recv,
            device_id=peer(o, other), device_id_type=MESH)

    for o, other in peers:
        s_copy(o, other, tp).start()
    inbox[tp] = msg[0]
    others = inbox.at[pl.ds(0, len(peers))]
    everything = pltpu.make_async_remote_copy(
        src_ref=others, dst_ref=others, send_sem=s_send, recv_sem=s_recv,
        device_id=peer(1, False), device_id_type=MESH)
    everything.wait_recv()

    def combine(x):
        m = jnp.max(x[:, 0:1, :], axis=0)
        r = lax.broadcasted_iota(jnp.int32, x.shape, 1)
        weight = jnp.exp2(x[:, 0:1, :] - m[None])
        s = jnp.sum(jnp.where((r == 1) | (r == 2), x * weight, x), axis=0)
        return m, s

    m, s = combine(inbox[0:tp_size])
    if PAIRED:
        m2, s2 = combine(inbox[tp_size:])
        m2 = pltpu.roll(jnp.broadcast_to(m2, (8, 128)), OTHER, 1)[0:1]
        s2 = pltpu.roll(s2, OTHER, 1)
        top = jnp.maximum(m, m2)
        r = lax.broadcasted_iota(jnp.int32, s.shape, 0)
        ours, theirs = jnp.exp2(m - top), jnp.exp2(m2 - top)
        scaled = (r == 1) | (r == 2)
        s = jnp.where(scaled, s * ours, s) + jnp.where(scaled, s2 * theirs, s2)
        m = top
    lse = m * LN2 + jnp.log(s[1:2])
    ent = lse - LN2 * (s[2:3] / s[1:2])
    lp = LN2 * s[3:4] - lse

    if PAIRED:
        p_copy.wait_send()
    vecs[0:1, :] = lse
    vecs[1:2, :] = ent
    vecs[2:3, :] = lp
    out_ref[...] = vecs[...]

    everything.wait_send()
    if PAIRED:
        g_copy.wait_send()
        f_copy.wait_send()


def unpack(lines_ref, lp_ref, lse_ref, ent_ref):
    batch, width = lse_ref.shape
    for b in range(batch):
        line = pltpu.roll(lines_ref[...], (128 - b * width) % 128, 1)
        lse_ref[b : b + 1, :] = line[0:1, :width]
        ent_ref[b : b + 1, :] = line[1:2, :width]
        lp_ref[b : b + 1, :] = line[2:3, : lp_ref.shape[1]]


def solution(mesh):
    tp_size = mesh.shape["tp"]

    def local_step(hidden, draft_ids, temperature, norm_gain, head_shard):
        batch, width, dim = hidden.shape
        shard_rows = head_shard.shape[0]
        short = shard_rows % CHUNK
        first_rows = (short // 3, short - short // 3)
        n_own = OWN_CHUNKS
        share_rows = (shard_rows - short - n_own * CHUNK) // 2
        n_late = -(-share_rows // CHUNK)
        last_rows = share_rows - (n_late - 1) * CHUNK
        n_all = 2 + n_own + n_late
        late = n_own + 2
        blocks = [[0], [1]] + BLOCKS_OWN + [[late + i for i in x] for x in BLOCKS_LATE]
        vmem, dma = pltpu.VMEM, pltpu.SemaphoreType.DMA
        f32, bf16 = jnp.float32, jnp.bfloat16
        any_space = pl.BlockSpec(memory_space=pltpu.HBM)
        out = pl.BlockSpec(memory_space=pltpu.VMEM)
        lines = pl.pallas_call(
            functools.partial(kernel, tp_size, blocks, n_own, n_all, last_rows, first_rows, share_rows),
            out_shape=pltpu.VMEM((8, 128), f32),
            in_specs=[any_space] * 5,
            out_specs=out,
            scratch_shapes=[
                pltpu.SMEM(draft_ids.shape, jnp.int32),
                pltpu.SMEM(temperature.shape, f32),
                vmem(hidden.shape, bf16),
                vmem((dim,), bf16),
                vmem((2, batch * width * (dim // 256), 128), f32),
                vmem((2, batch * width * (dim // 256), 128), f32),
                vmem((128, dim), bf16),
                vmem((SLOTS, CHUNK, dim), bf16),
                vmem((4, CHUNK, 128), f32),
                vmem((8, 128), f32),
                vmem((8, 128), jnp.int32),
                vmem((8, 128), f32),
                vmem((4, 8, 128), f32),
                vmem((2, 8, 128), f32),
                vmem((2 * tp_size, 8, 128), f32),
                dma((4,)), dma((SLOTS + 1,)),
                dma, dma, dma, dma, dma, dma((2,)),
                dma, dma,
            ],
            compiler_params=pltpu.CompilerParams(
                collective_id=0, has_side_effects=True, vmem_limit_bytes=60 * 2**20),
        )(hidden, draft_ids, temperature, norm_gain, head_shard)
        return pl.pallas_call(
            unpack,
            out_shape=(
                jax.ShapeDtypeStruct(draft_ids.shape, f32),
                jax.ShapeDtypeStruct((batch, width), f32),
                jax.ShapeDtypeStruct((batch, width), f32),
            ),
            in_specs=[out],
            out_specs=(out, out, out),
        )(pltpu.with_memory_space_constraint(lines, pltpu.VMEM))

    return jax.shard_map(
        local_step,
        mesh=mesh,
        in_specs=(P("dp", None, None), P("dp", None), P("dp"), P(None), P("tp", None)),
        out_specs=(P("dp", None), P("dp", None), P("dp", None)),
        check_vma=False,
    )
```

```python
import functools

import jax
import jax.numpy as jnp
from jax import lax
from jax.experimental import pallas as pl
from jax.experimental.pallas import tpu as pltpu
from jax.sharding import PartitionSpec as P

NORM_EPS = 1e-5
MESH = pl.DeviceIdType.MESH
LOW = -3.4e38
CHUNK = 1024
SLOTS = 6
OTHER = 64
PAIRED = True
BLOCKS_OWN = [[2], [3], [4]]
BLOCKS_LATE = [[0], [1], [2], [3], [4], [5]]
OWN_CHUNKS = 3


def kernel(
    tp_size, blocks, n_own, n_all, last_rows, first_rows, share_rows,
    hidden_hbm, draft_hbm, temp_hbm, gain_hbm, w_hbm,
    out_ref,
    draft_ref, temp_ref, hv, gv, gs, gr, g2, buf, zs, vecs, ids_v, vecs_r, stats, msg, inbox,
    in_sem, w_sem, g_send, g_recv, p_send, p_recv, f_send, f_recv, s_send, s_recv,
):
    dp, tp = lax.axis_index("dp"), lax.axis_index("tp")
    half = lax.rem(dp, 2)
    mate = dp + 1 - 2 * half
    core = lax.rem(tp, 2)
    twin = tp + 1 - 2 * core
    shard_rows, dim = w_hbm.shape
    batch, width = hidden_hbm.shape[:2]
    draft_len = draft_hbm.shape[1]
    hd = dim // 2

    def peer(o, other):
        return (mate if other else dp, lax.rem(tp + o, tp_size))

    far_first = sorted(range(tp_size), key=lambda o: -min(o, tp_size - o))
    peers = [(o, True) for o in far_first] if PAIRED else []
    peers += [(o, False) for o in far_first if o]

    own_rows = first_rows[0] + first_rows[1] + n_own * CHUNK
    shared_base = own_rows + half * share_rows if PAIRED else own_rows

    def chunk(j):
        if j == 0:
            return 0, first_rows[0], 0, 0
        if j == 1:
            return first_rows[0], first_rows[1], 0, first_rows[0]
        rows = last_rows if j == n_all - 1 else CHUNK
        early = first_rows[0] + first_rows[1] + (j - 2) * CHUNK
        if j - 2 < n_own:
            return early, rows, (j - 1) % SLOTS, 0
        return shared_base + (j - 2 - n_own) * CHUNK, rows, (j - 1) % SLOTS, 0

    def w_copy(j):
        row, rows, slot, at = chunk(j)
        if not isinstance(row, int):
            row = pl.multiple_of(row, 16)
        return pltpu.make_async_copy(
            w_hbm.at[pl.ds(row, rows)], buf.at[slot, pl.ds(at, rows)], w_sem.at[0 if j == 0 else slot + 1])

    h_copy = pltpu.make_async_copy(hidden_hbm, hv, in_sem.at[0])
    gain_copy = pltpu.make_async_copy(gain_hbm, gv, in_sem.at[1])
    draft_copy = pltpu.make_async_copy(draft_hbm, draft_ref, in_sem.at[2])
    temp_copy = pltpu.make_async_copy(temp_hbm, temp_ref, in_sem.at[3])
    h_copy.start()
    gain_copy.start()
    draft_copy.start()
    temp_copy.start()
    for j in range(SLOTS + 1):
        w_copy(j).start(priority=1)

    barrier = pltpu.get_barrier_semaphore()
    for o, other in peers:
        pl.semaphore_signal(barrier, inc=1, device_id=peer(o, other), device_id_type=MESH)

    draft_copy.wait()
    temp_copy.wait()
    lane = lax.broadcasted_iota(jnp.int32, (1, 128), 1)
    scale = jnp.zeros((1, 128), jnp.float32)
    ids = jnp.full((1, 128), -1, jnp.int32)
    for b in range(batch):
        inside = (lane >= b * width) & (lane < (b + 1) * width)
        scale = jnp.where(inside, temp_ref[b], scale)
        for i in range(draft_len):
            ids = jnp.where(lane == b * width + i, draft_ref[b, i], ids)
    scale = jnp.where(lane < batch * width, 1.0 / jnp.where(scale == 0.0, 1.0, scale), 0.0)
    vecs[...] = jnp.zeros_like(vecs)
    vecs[0:1, :] = scale
    vecs[1:2, :] = ids.astype(jnp.float32)
    ids_v[...] = jnp.broadcast_to(ids, (8, 128))
    stats[0] = jnp.full((8, 128), LOW, jnp.float32)
    stats[1] = jnp.zeros((8, 128), jnp.float32)
    stats[2] = jnp.zeros((8, 128), jnp.float32)
    stats[3] = jnp.zeros((8, 128), jnp.float32)
    g2[...] = jnp.zeros_like(g2)

    h_copy.wait()
    gain_copy.wait()
    gain = gv[...].astype(jnp.float32).reshape(1, dim)
    n_pos, n_k = batch * width, hd // 128

    def place(src, h, row):
        for k in range(n_k):
            ks = pl.ds(pl.multiple_of(h * hd + k * 128, 128), 128)
            g2[row : row + n_pos, ks] = src[h, pl.ds(k, n_pos, stride=n_k), :].astype(jnp.bfloat16)

    for b in range(batch):
        hb = hv[b].astype(jnp.float32)
        mean_sq = jnp.sum(hb * hb, axis=-1, keepdims=True) * (1.0 / dim)
        g = (hb * lax.rsqrt(mean_sq + NORM_EPS) * gain).astype(jnp.bfloat16).astype(jnp.float32)
        for c in range(2):
            for k in range(n_k):
                at = c * hd + k * 128
                gs[c, pl.ds(b * width * n_k + k, width, stride=n_k), :] = g[:, at : at + 128]
    for c in range(2):
        place(gs, c, 0)

    g_copy = pltpu.make_async_remote_copy(
        src_ref=gs.at[core], dst_ref=gr.at[core], send_sem=g_send, recv_sem=g_recv,
        device_id=(mate, tp), device_id_type=MESH)
    p_copy = pltpu.make_async_remote_copy(
        src_ref=vecs, dst_ref=vecs_r, send_sem=p_send, recv_sem=p_recv,
        device_id=(mate, tp), device_id_type=MESH)
    f_copy = pltpu.make_async_remote_copy(
        src_ref=gr.at[core], dst_ref=gr.at[core], send_sem=f_send, recv_sem=f_recv.at[core],
        device_id=(dp, twin), device_id_type=MESH)
    f_wait = pltpu.make_async_remote_copy(
        src_ref=gr.at[1 - core], dst_ref=gr.at[1 - core], send_sem=f_send, recv_sem=f_recv.at[1 - core],
        device_id=(dp, twin), device_id_type=MESH)
    def forward():
        g_copy.wait_recv()
        f_copy.start()

    def join(h):
        place(gr, h, OTHER)

    def join_lanes():
        p_copy.wait_recv()
        theirs = lane >= OTHER
        v = pltpu.roll(vecs_r[...], OTHER, 1)
        scale_all[...] = jnp.where(theirs, v[0:1], scale_all[...])
        ids_v[...] = jnp.where(theirs, jnp.broadcast_to(v[1:2].astype(jnp.int32), (8, 128)), ids_v[...])
        stats[0] = jnp.where(theirs, LOW, stats[0])
        for r in range(1, 4):
            stats[r] = jnp.where(theirs, 0.0, stats[r])

    scale_all = msg.at[1]
    scale_all[...] = jnp.broadcast_to(scale, (8, 128))

    def epilogue(z, base):
        rows = z.shape[0]
        z = z.reshape(rows // 8, 8, 128) * scale_all[...][None]
        old = stats[0]
        new = jnp.maximum(old, jnp.max(z, axis=0))
        e = jnp.exp(z - new[None])
        fix = jnp.exp(old - new)
        stats[0] = new
        stats[1] = stats[1] * fix + jnp.sum(e, axis=0)
        stats[2] = stats[2] * fix + jnp.sum(e * z, axis=0)
        row = lax.broadcasted_iota(jnp.int32, z.shape, 0) * 8 + lax.broadcasted_iota(jnp.int32, z.shape, 1)
        hit = row == (ids_v[...] - (tp * shard_rows + base))[None]
        stats[3] = stats[3] + jnp.sum(jnp.where(hit, z, 0.0), axis=0)

    def product(j):
        _, rows, slot, at = chunk(j)
        part = rows // 2
        return [
            lax.dot_general(
                buf[slot, at + q * part : at + (q + 1) * part], g2[...],
                (((1,), (1,)), ((), ())), preferred_element_type=jnp.float32)
            for q in range(2)
        ]

    def half_product(j, h):
        _, rows, slot, at = chunk(j)
        part = rows // 2
        ks = pl.ds(pl.multiple_of(h * hd, 128), hd)
        return [
            lax.dot_general(
                buf[slot, pl.ds(at + q * part, part), ks], g2[:, ks],
                (((1,), (1,)), ((), ())), preferred_element_type=jnp.float32)
            for q in range(2)
        ]

    def drain(done):
        for j, z in done:
            base, rows = chunk(j)[:2]
            part = rows // 2
            for q in range(2):
                epilogue(zs[z, q * part : (q + 1) * part], base + q * part)

    done = []
    for n, block in enumerate(blocks):
        forwarding = PAIRED and block[0] == n_own + 1
        joining = PAIRED and block[0] == n_own + 2
        if joining:
            join(core)
        for j in block:
            w_copy(j).wait()
        if n == 0:
            pl.semaphore_wait(barrier, len(peers))
            if PAIRED:
                g_copy.start()
                p_copy.start()
        if forwarding or joining:
            first = half_product(block[0], core)
            if forwarding:
                z = 2 * (n % 2)
                for q in range(2):
                    zs[z, q * (CHUNK // 2) : (q + 1) * (CHUNK // 2)] = first[q]
                forward()
                second = half_product(block[0], 1 - core)
                first = [zs[z, q * (CHUNK // 2) : (q + 1) * (CHUNK // 2)] for q in range(2)]
            else:
                drain(done)
                done = []
                z = 2 * (n % 2)
                for q in range(2):
                    zs[z, q * (CHUNK // 2) : (q + 1) * (CHUNK // 2)] = first[q]
                f_wait.wait_recv()
                join(1 - core)
                second = half_product(block[0], 1 - core)
                first = [zs[z, q * (CHUNK // 2) : (q + 1) * (CHUNK // 2)] for q in range(2)]
            parts = [[x + y for x, y in zip(first, second)]]
        else:
            parts = [product(j) for j in block]
        drain(done)
        done = [(j, 2 * (n % 2) + i) for i, j in enumerate(block)]
        for (j, z), p in zip(done, parts):
            rows = p[0].shape[0]
            for q in range(2):
                zs[z, q * rows : (q + 1) * rows] = p[q]
        if joining:
            join_lanes()
        for j in block:
            if 1 <= j and j + SLOTS < n_all:
                w_copy(j + SLOTS).start(priority=1)
    drain(done)

    m8 = stats[0]
    m1 = jnp.max(m8, axis=0, keepdims=True)
    w8 = jnp.exp(m8 - m1)
    out = msg.at[0]
    out[4:8, :] = jnp.zeros((4, 128), jnp.float32)
    out[0:1, :] = m1
    out[1:2, :] = jnp.sum(stats[1] * w8, axis=0, keepdims=True)
    out[2:3, :] = jnp.sum(stats[2] * w8, axis=0, keepdims=True)
    out[3:4, :] = jnp.sum(stats[3], axis=0, keepdims=True)

    def s_copy(o, other, source):
        i = 1 if other else 0
        return pltpu.make_async_remote_copy(
            src_ref=msg.at[0], dst_ref=inbox.at[i * tp_size + source], send_sem=s_send, recv_sem=s_recv,
            device_id=peer(o, other), device_id_type=MESH)

    for o, other in peers:
        s_copy(o, other, tp).start()
    inbox[tp] = msg[0]
    others = inbox.at[pl.ds(0, len(peers))]
    everything = pltpu.make_async_remote_copy(
        src_ref=others, dst_ref=others, send_sem=s_send, recv_sem=s_recv,
        device_id=peer(1, False), device_id_type=MESH)
    everything.wait_recv()

    def combine(x):
        m = jnp.max(x[:, 0:1, :], axis=0)
        r = lax.broadcasted_iota(jnp.int32, x.shape, 1)
        weight = jnp.exp(x[:, 0:1, :] - m[None])
        s = jnp.sum(jnp.where((r == 1) | (r == 2), x * weight, x), axis=0)
        return m, s

    m, s = combine(inbox[0:tp_size])
    if PAIRED:
        m2, s2 = combine(inbox[tp_size:])
        m2 = pltpu.roll(jnp.broadcast_to(m2, (8, 128)), OTHER, 1)[0:1]
        s2 = pltpu.roll(s2, OTHER, 1)
        top = jnp.maximum(m, m2)
        r = lax.broadcasted_iota(jnp.int32, s.shape, 0)
        ours, theirs = jnp.exp(m - top), jnp.exp(m2 - top)
        scaled = (r == 1) | (r == 2)
        s = jnp.where(scaled, s * ours, s) + jnp.where(scaled, s2 * theirs, s2)
        m = top
    lse = m + jnp.log(s[1:2])
    ent = lse - (s[2:3] / s[1:2])
    lp = s[3:4] - lse

    if PAIRED:
        p_copy.wait_send()
    vecs[0:1, :] = lse
    vecs[1:2, :] = ent
    vecs[2:3, :] = lp
    out_ref[...] = vecs[...]

    everything.wait_send()
    if PAIRED:
        g_copy.wait_send()
        f_copy.wait_send()


def unpack(lines_ref, lp_ref, lse_ref, ent_ref):
    batch, width = lse_ref.shape
    for b in range(batch):
        line = pltpu.roll(lines_ref[...], (128 - b * width) % 128, 1)
        lse_ref[b : b + 1, :] = line[0:1, :width]
        ent_ref[b : b + 1, :] = line[1:2, :width]
        lp_ref[b : b + 1, :] = line[2:3, : lp_ref.shape[1]]


def solution(mesh):
    tp_size = mesh.shape["tp"]

    def local_step(hidden, draft_ids, temperature, norm_gain, head_shard):
        batch, width, dim = hidden.shape
        shard_rows = head_shard.shape[0]
        short = shard_rows % CHUNK
        first_rows = (short // 3, short - short // 3)
        n_own = OWN_CHUNKS
        share_rows = (shard_rows - short - n_own * CHUNK) // 2
        n_late = -(-share_rows // CHUNK)
        last_rows = share_rows - (n_late - 1) * CHUNK
        n_all = 2 + n_own + n_late
        late = n_own + 2
        blocks = [[0], [1]] + BLOCKS_OWN + [[late + i for i in x] for x in BLOCKS_LATE]
        vmem, dma = pltpu.VMEM, pltpu.SemaphoreType.DMA
        f32, bf16 = jnp.float32, jnp.bfloat16
        any_space = pl.BlockSpec(memory_space=pltpu.HBM)
        out = pl.BlockSpec(memory_space=pltpu.VMEM)
        lines = pl.pallas_call(
            functools.partial(kernel, tp_size, blocks, n_own, n_all, last_rows, first_rows, share_rows),
            out_shape=pltpu.VMEM((8, 128), f32),
            in_specs=[any_space] * 5,
            out_specs=out,
            scratch_shapes=[
                pltpu.SMEM(draft_ids.shape, jnp.int32),
                pltpu.SMEM(temperature.shape, f32),
                vmem(hidden.shape, bf16),
                vmem((dim,), bf16),
                vmem((2, batch * width * (dim // 256), 128), f32),
                vmem((2, batch * width * (dim // 256), 128), f32),
                vmem((128, dim), bf16),
                vmem((SLOTS, CHUNK, dim), bf16),
                vmem((4, CHUNK, 128), f32),
                vmem((8, 128), f32),
                vmem((8, 128), jnp.int32),
                vmem((8, 128), f32),
                vmem((4, 8, 128), f32),
                vmem((2, 8, 128), f32),
                vmem((2 * tp_size, 8, 128), f32),
                dma((4,)), dma((SLOTS + 1,)),
                dma, dma, dma, dma, dma, dma((2,)),
                dma, dma,
            ],
            compiler_params=pltpu.CompilerParams(
                collective_id=0, has_side_effects=True, vmem_limit_bytes=60 * 2**20),
        )(hidden, draft_ids, temperature, norm_gain, head_shard)
        return pl.pallas_call(
            unpack,
            out_shape=(
                jax.ShapeDtypeStruct(draft_ids.shape, f32),
                jax.ShapeDtypeStruct((batch, width), f32),
                jax.ShapeDtypeStruct((batch, width), f32),
            ),
            in_specs=[out],
            out_specs=(out, out, out),
        )(pltpu.with_memory_space_constraint(lines, pltpu.VMEM))

    return jax.shard_map(
        local_step,
        mesh=mesh,
        in_specs=(P("dp", None, None), P("dp", None), P("dp"), P(None), P("tp", None)),
        out_specs=(P("dp", None), P("dp", None), P("dp", None)),
        check_vma=False,
    )
```
